32 devices in a mesh: space: 16 (over z, y, x), level: 2 (over core).
Axes of the slice: x: 2, y: 2, z: 4, core: 2. Of those that a mesh axis runs over, the one named last changes fastest.
Arguments:
- velocity: float32 [2, 16, 16384], P(None, 'level', 'space'), may hold values from -3 to 3
- density: float32 [16, 16384], P('level', 'space'), may hold values from -6 to 6
- elevation: float32 [16384], P('space'), may hold values from -3 to 3
- grad_weights: float32 [2, 6, 16384], P(None, None, 'space'), may hold values from -2.4 to 2.4
- lap_weights: float32 [6, 16384], P(None, 'space'), may hold values from 0.02 to 0.2
- coriolis: float32 [16384], P('space'), may hold values from 0.5 to 2
- node_area: float32 [16384], P('space'), may hold values from 1 to 100, as said below
- thickness: float32 [16], P('level'), may hold values from 0.5 to 2
- send_list: int32 [16, 256], P('space'), may hold values from 0 to 1023
- neighbours: int32 [6, 16384], P(None, 'space'), may hold values from 0 to 1279
- bottom: int32 [16384], P('space'), may hold values from 0 to 16, as said below
Outputs:
- velocity_out: float32 [2, 16, 16384], P(None, 'level', 'space')
- density_out: float32 [16, 16384], P('level', 'space')
- elevation_out: float32 [16384], P('space')
- volume_drift: float32 [4], replicated
The draws below stay inside these ranges and needn't reach their ends.
Inputs may be any that keep to these rules, and one draw needn't show every extreme that they name: `send_list`: local node numbers within the sending partition; the first 128 go to the partition one below along space, the other 128 to the one above. `neighbours`: slots below 1024 are the partition's own nodes; the next 128 are halo slots filled from the partition below, the last 128 from the partition above. Levels of a node are wet from the surface down to bottom - 1; a node with 0 is dry. Some partitions are shallower than others. `node_area`: positive areas.
All inputs are finite; a program needn't handle non-finite values.
Results may differ from the reference program's by a relative error of at most 0.00013.
Values sent between devices are 32-bit elements; how exact they have to be, the bound alone decides.
No kernel may reach another device: no remote copies, remote signals or barrier semaphores. Data moves between devices by JAX's collectives and lax.ppermute only.
A program may use at most 64 MiB of HBM per device.

```python
import math
import jax
import jax.numpy as jnp
from jax import lax

NODES_DEV = 1024
HALO = 128
K = 6
STEPS = 4
NODES = 16384
LEVELS = 16
N_SPACE = 16


def draw_bottom(key, part):
    key_part = jax.random.fold_in(key, 11)
    key_node = jax.random.fold_in(key, 12)
    partitions = NODES // NODES_DEV
    shallow = jax.random.randint(key_part, (partitions, 1), LEVELS // 4, LEVELS + 1)
    shallow = shallow.at[0].set(LEVELS)
    depths = jax.random.randint(key_node, (partitions, NODES_DEV), 0, LEVELS + 1)
    return jnp.minimum(depths, shallow).reshape(NODES).astype(jnp.int32)


def draw_node_area(key, part):
    key_rough = jax.random.fold_in(key, 21)
    partitions = NODES // NODES_DEV
    owner = (jnp.arange(NODES, dtype=jnp.int32) // NODES_DEV).astype(jnp.float32)
    position = owner / jnp.float32(max(partitions - 1, 1))
    ramp = jnp.exp(jnp.log(jnp.float32(10.0)) * position)
    rough = jnp.exp(jax.random.uniform(key_rough, (NODES,), jnp.float32, 0.0, jnp.log(3.0)))
    return (ramp * rough).astype(jnp.float32)


def plant(values, rng, smallest, high):
    spot = [jax.random.randint(jax.random.fold_in(rng, axis), (), 0, length) for axis, length in enumerate(values.shape)]
    longest = values.shape.index(max(values.shape))
    neighbour = spot[:longest] + [(spot[longest] + 1) % values.shape[longest]] + spot[longest + 1:]
    return values.at[tuple(spot)].set(smallest).at[tuple(neighbour)].set(high)


def block_levels(rng, extent, pieces, smallest, top_value):
    loudness, own = 1.0, jax.random.fold_in(rng, 6)
    for dim, blocks in pieces:
        heights = jnp.exp(jax.random.uniform(jax.random.fold_in(own, dim), (blocks,), jnp.float32, smallest / len(pieces), top_value / len(pieces)))
        loudness = loudness * jnp.repeat(heights, extent[dim] // blocks).reshape([-1 if axis == dim else 1 for axis in range(len(extent))])
    return loudness


def scatter_about(rng, shape, width, most, shards=(), held_as=jnp.bfloat16):
    loudness = block_levels(rng, shape, shards, -0.22, 0.18) if shards else 1.0
    values = jax.random.normal(rng, shape, jnp.float32) * width * loudness
    return jnp.minimum(jnp.maximum(values, -most), most).astype(held_as)


def setup_inputs(seed: int = 0) -> dict:
    key_list = jax.random.split(jax.random.key(seed), 12)
    return {
        "velocity": scatter_about(key_list[0], (2, LEVELS, NODES), 0.5, 3.0, ((1, 2), (2, 16)), jnp.float32),
        "density": scatter_about(key_list[1], (LEVELS, NODES), 1.0, 6.0, ((0, 2), (1, 16)), jnp.float32),
        "elevation": scatter_about(key_list[2], (NODES,), 0.5, 3.0, ((0, 16),), jnp.float32),
        "grad_weights": scatter_about(key_list[3], (2, K, NODES), 0.4, 2.4, ((2, 16),), jnp.float32),
        "lap_weights": jnp.clip(jnp.exp(math.log(0.2) - 2.3025851 * jax.random.uniform(key_list[4], (K, NODES), jnp.float32) ** block_levels(key_list[4], (K, NODES), ((1, 16),), -0.2, 0.2)), 0.02, 0.2),
        "coriolis": jnp.clip(jnp.exp(math.log(2.0) - 1.3862944 * jax.random.uniform(key_list[5], (NODES,), jnp.float32) ** block_levels(key_list[5], (NODES,), ((0, 16),), -0.2, 0.2)), 0.5, 2.0),
        "node_area": draw_node_area(jax.random.fold_in(key_list[11], 71), 0),
        "thickness": jnp.clip(jnp.exp(math.log(2.0) - 1.3862944 * jax.random.uniform(key_list[7], (LEVELS,), jnp.float32) ** block_levels(key_list[7], (LEVELS,), ((0, 2),), -0.2, 0.2)), 0.5, 2.0),
        "send_list": plant(jax.random.randint(key_list[8], (N_SPACE, 2 * HALO), 0, NODES_DEV), jax.random.fold_in(key_list[8], 1), 0, NODES_DEV - 1).astype(jnp.int32),
        "neighbours": plant(jax.random.randint(key_list[9], (K, NODES), 0, NODES_DEV + 2 * HALO), jax.random.fold_in(key_list[9], 1), 0, (NODES_DEV + 2 * HALO) - 1).astype(jnp.int32),
        "bottom": draw_bottom(jax.random.fold_in(key_list[11], 71), 0),
    }


time_step = 0.1
buoyancy = 0.5
drag_rate = 0.5


def neighbour_table(send_list, neighbours):
    node_ids = jnp.arange(NODES, dtype=jnp.int32)
    owner = (node_ids // NODES_DEV)[None, :]
    slot_index = neighbours
    source_below = jnp.clip(owner - 1, 0, N_SPACE - 1)
    source_above = jnp.clip(owner + 1, 0, N_SPACE - 1)
    local_below = send_list[source_below, jnp.clip(HALO + slot_index - NODES_DEV, 0, 2 * HALO - 1)]
    local_above = send_list[source_above, jnp.clip(slot_index - NODES_DEV - HALO, 0, 2 * HALO - 1)]
    global_index = jnp.where(slot_index < NODES_DEV, owner * NODES_DEV + slot_index,
                             jnp.where(slot_index < NODES_DEV + HALO, source_below * NODES_DEV + local_below,
                                       source_above * NODES_DEV + local_above))
    is_valid = jnp.where(slot_index < NODES_DEV, True,
                         jnp.where(slot_index < NODES_DEV + HALO, owner >= 1, owner <= N_SPACE - 2))
    return global_index.astype(jnp.int32), is_valid.astype(jnp.float32)


def stencil(fields, global_index, weight):
    result = jnp.zeros_like(fields)
    for column in range(K):
        nearby = jnp.take(fields, global_index[column], axis=-1)
        result = result + weight[column] * (nearby - fields)
    return result


def reference(velocity, density, elevation, grad_weights, lap_weights, coriolis, node_area, thickness, send_list, neighbours, bottom):
    global_index, valid_float = neighbour_table(send_list, neighbours)
    east_weight = grad_weights[0] * valid_float
    north_weight = grad_weights[1] * valid_float
    smooth_weight = lap_weights * valid_float
    level_ids = jnp.arange(LEVELS, dtype=jnp.int32)[:, None]
    wet_cells = (level_ids < bottom[None, :]).astype(jnp.float32)
    at_floor = (level_ids == bottom[None, :] - 1).astype(jnp.float32)
    wet_nodes = (bottom > 0).astype(jnp.float32)
    area_total = jnp.sum(node_area * wet_nodes)
    velocity = velocity * wet_cells[None]
    drifts = []
    for counter in range(STEPS):
        east_speed = velocity[0]
        north_speed = velocity[1]
        weighted = density * thickness[:, None]
        pressure = buoyancy * (jnp.cumsum(weighted, axis=0) - 0.5 * weighted)
        transport = jnp.einsum('cln,l->cn', velocity, thickness, precision=lax.Precision.HIGHEST)
        diverge = stencil(transport[0], global_index, east_weight) + stencil(transport[1], global_index, north_weight)
        drift = jnp.sum(node_area * wet_nodes * diverge) / area_total
        drifts.append(drift)
        new_elevation = elevation - time_step * wet_nodes * diverge + time_step * drift
        slope_east = stencil(elevation, global_index, east_weight)
        slope_north = stencil(elevation, global_index, north_weight)
        press_east = stencil(pressure, global_index, east_weight)
        press_north = stencil(pressure, global_index, north_weight)
        smooth_speed = stencil(velocity.reshape(2 * LEVELS, NODES), global_index, smooth_weight)
        push_east = (-slope_east[None] - press_east + coriolis[None] * north_speed
                     + smooth_speed[:LEVELS] - drag_rate * at_floor * east_speed)
        push_north = (-slope_north[None] - press_north - coriolis[None] * east_speed
                      + smooth_speed[LEVELS:] - drag_rate * at_floor * north_speed)
        dense_east = stencil(density, global_index, east_weight)
        dense_north = stencil(density, global_index, north_weight)
        dense_smooth = stencil(density, global_index, smooth_weight)
        density = density + time_step * (dense_smooth - east_speed * dense_east - north_speed * dense_north)
        velocity = wet_cells[None] * (velocity + time_step * jnp.stack([push_east, push_north]))
        elevation = new_elevation
    return velocity, density, elevation, jnp.stack(drifts).astype(jnp.float32)
```

```python
import jax
import jax.numpy as jnp
from jax import lax
from jax.experimental import pallas as pl
from jax.experimental.pallas import tpu as pltpu
from jax.sharding import PartitionSpec as P

STEPS = 4

time_step = 0.1
buoyancy = 0.5
drag_rate = 0.5

LANES = 128
SUBS = 8


def lane_gather(source, lane):
    return lax.gather(
        source,
        lane[..., None],
        lax.GatherDimensionNumbers(
            offset_dims=(),
            collapsed_slice_dims=(1,),
            start_index_map=(1,),
            operand_batching_dims=(0,),
            start_indices_batching_dims=(0,),
        ),
        slice_sizes=(1, 1),
        mode=lax.GatherScatterMode.PROMISE_IN_BOUNDS,
    )


def spread(row, rows=SUBS):
    return jnp.broadcast_to(row, (rows, row.shape[1]))


def level_prefix(value):
    sub = lax.broadcasted_iota(jnp.int32, (SUBS, LANES), 0)
    out, carry = [], None
    for block in value:
        shift = 1
        while shift < SUBS:
            block = block + jnp.where(sub >= shift, pltpu.roll(block, shift, 0), 0.0)
            shift *= 2
        if carry is not None:
            block = block + carry
        carry = spread(block[SUBS - 1 :])
        out.append(block)
    return out


def pick(sources, lane, block):
    out = None
    for number, rows in enumerate(sources):
        here = [lane_gather(row(), lane) for row in rows]
        if out is None:
            out = here
        else:
            match = block == number
            out = [jnp.where(match, new, old) for new, old in zip(here, out)]
    return out


def send_out(state, eta, send, outgoing):
    rows, node_count = state.shape
    half = send.shape[1] // 2
    for side in range(2):
        for chunk in range(half // LANES):
            first = side * half + chunk * LANES
            ids = spread(send[0:1, first : first + LANES])
            sources = []
            for number in range(node_count // LANES):
                cols = slice(number * LANES, (number + 1) * LANES)
                own = [
                    lambda g=g, cols=cols: state[g : g + SUBS, cols]
                    for g in range(0, rows, SUBS)
                ]
                own.append(lambda cols=cols: spread(eta[0:1, cols]))
                sources.append(own)
            found = pick(sources, ids & (LANES - 1), ids >> 7)
            for g, block in enumerate(found):
                outgoing[
                    side, g * SUBS : (g + 1) * SUBS, chunk * LANES : (chunk + 1) * LANES
                ] = block


def begin_kernel(parts, eta, bottom, node_area, send, state, outgoing, volume):
    shards, held, width = parts.shape
    fields, node_count = 3, eta.shape[1]
    level_count = shards * held
    area = jnp.where(bottom[0:1, :] > 0, node_area[0:1, :], 0.0)
    area = sum(area[:, i : i + LANES] for i in range(0, node_count, LANES))
    sub = lax.broadcasted_iota(jnp.int32, (SUBS, LANES), 0)
    volume[...] = jnp.where(sub == STEPS, spread(area), 0.0)
    for shard in range(shards):
        ids = lax.broadcasted_iota(jnp.int32, (held, node_count), 0) + shard * held
        wet = ids < jnp.broadcast_to(bottom[0:1, :], (held, node_count))
        for field in range(fields):
            value = parts[shard, :, field * node_count : (field + 1) * node_count]
            if field < 2:
                value = jnp.where(wet, value, 0.0)
            first = field * level_count + shard * held
            state[first : first + held, :] = value
    send_out(state, eta, send, outgoing)


def step_kernel(
    edges,
    volume_in,
    state,
    eta,
    first_halo,
    second_halo,
    neighbours,
    weights,
    coriolis,
    node_area,
    bottom,
    thickness,
    send,
    new_state,
    new_eta,
    outgoing,
    volume,
    *,
    near_count,
    step,
):
    rows, node_count = state.shape
    half = first_halo.shape[1]
    level_count = rows // 3
    groups = level_count // SUBS
    slots = (node_count, node_count + half)
    first_ok, second_ok = edges[0], edges[1]

    def source_blocks():
        for ref, width in ((state, node_count), (first_halo, half), (second_halo, half)):
            for number in range(width // LANES):
                cols = slice(number * LANES, (number + 1) * LANES)
                yield ref, cols

    eta_sources, state_sources = [], []
    for ref, cols in source_blocks():
        eta_ref, eta_row = (eta, 0) if ref is state else (ref, rows)
        eta_sources.append(
            [lambda r=eta_ref, i=eta_row, c=cols: spread(r[i : i + 1, c])]
        )
        state_sources.append(
            [lambda r=ref, g=g, c=cols: r[g : g + SUBS, c] for g in range(0, rows, SUBS)]
        )

    sub = lax.broadcasted_iota(jnp.int32, (SUBS, LANES), 0)

    def tile(number, total):
        cols = pl.ds(pl.multiple_of(number * LANES, LANES), LANES)
        ids = neighbours[:, cols]
        lanes, blocks = ids & (LANES - 1), ids >> 7
        valid = jnp.where(ids < slots[0], 1.0, jnp.where(ids < slots[1], first_ok, second_ok))
        east, north, smooth = (weights[i, :, cols] * valid for i in range(3))
        eta_here = eta[0:1, cols]
        (eta_near,) = pick(eta_sources, lanes, blocks)
        eta_differ = eta_near - spread(eta_here)
        slope_east = spread(jnp.sum(east * eta_differ, axis=0, keepdims=True))
        slope_north = spread(jnp.sum(north * eta_differ, axis=0, keepdims=True))

        own = [state[g : g + SUBS, cols] for g in range(0, rows, SUBS)]
        zero = jnp.zeros((SUBS, LANES), jnp.float32)
        lap = [zero] * (3 * groups)
        flow = [zero] * groups
        dense_east = [zero] * groups
        dense_north = [zero] * groups
        for k in range(near_count):
            found = pick(state_sources, spread(lanes[k : k + 1]), spread(blocks[k : k + 1]))
            e, n, w = (spread(x[k : k + 1]) for x in (east, north, smooth))
            differ = [near - here for near, here in zip(found, own)]
            for i, value in enumerate(differ):
                lap[i] = lap[i] + w * value
            for g in range(groups):
                flow[g] = flow[g] + (e * differ[g] + n * differ[groups + g])
                dense_east[g] = dense_east[g] + e * differ[2 * groups + g]
                dense_north[g] = dense_north[g] + n * differ[2 * groups + g]

        thick = [thickness[g * SUBS : (g + 1) * SUBS, :] for g in range(groups)]
        diverge = sum(thick[g] * flow[g] for g in range(groups))
        diverge = jnp.sum(diverge, axis=0, keepdims=True)
        depth = bottom[0:1, cols]
        wet_nodes = jnp.where(depth > 0, 1.0, 0.0)
        total = total + node_area[0:1, cols] * wet_nodes * diverge
        new_eta[0:1, cols] = eta_here - time_step * wet_nodes * diverge

        weighted_east = [t * x for t, x in zip(thick, dense_east)]
        weighted_north = [t * x for t, x in zip(thick, dense_north)]
        press_east = level_prefix(weighted_east)
        press_north = level_prefix(weighted_north)
        turn = spread(coriolis[0:1, cols])
        depth = spread(depth)
        for g in range(groups):
            u, v, rho = (own[f * groups + g] for f in range(3))
            level = sub + g * SUBS
            wet = level < depth
            drag = jnp.where(level == depth - 1, drag_rate, 0.0)
            push_east = (
                lap[g]
                - slope_east
                - buoyancy * (press_east[g] - 0.5 * weighted_east[g])
                + turn * v
                - drag * u
            )
            push_north = (
                lap[groups + g]
                - slope_north
                - buoyancy * (press_north[g] - 0.5 * weighted_north[g])
                - turn * u
                - drag * v
            )
            rho_new = rho + time_step * (
                lap[2 * groups + g] - u * dense_east[g] - v * dense_north[g]
            )
            u_new = jnp.where(wet, u + time_step * push_east, 0.0)
            v_new = jnp.where(wet, v + time_step * push_north, 0.0)
            for f, value in enumerate((u_new, v_new, rho_new)):
                first = (f * groups + g) * SUBS
                new_state[first : first + SUBS, cols] = value
        return total

    total = lax.fori_loop(
        0, node_count // LANES, tile, jnp.zeros((1, LANES), jnp.float32)
    )
    volume[...] = jnp.where(sub == step, spread(total), volume_in[...])
    send_out(new_state, new_eta, send, outgoing)


def vmem(count):
    return [pl.BlockSpec(memory_space=pltpu.VMEM)] * count


def shape(*dims):
    return jax.ShapeDtypeStruct(dims, jnp.float32)


def make_local(mesh):
    def local(
        velocity,
        density,
        elevation,
        grad_weights,
        lap_weights,
        coriolis,
        node_area,
        thickness,
        send_list,
        neighbours,
        bottom,
    ):
        held, node_count = density.shape
        near_count = neighbours.shape[0]
        half = send_list.shape[1] // 2
        shards = mesh.shape["level"]
        space_count = mesh.shape["space"]
        level_count = shards * held
        rows = 3 * level_count
        space_rank = lax.axis_index("space")
        level_rank = lax.axis_index("level")
        ends = space_count - 1
        rounds = [
            [(i, j if 0 <= j <= ends else i) for i, j in pairs]
            for pairs in (
                [(i, i ^ 1) for i in range(space_count)],
                [(i, ((i + 1) ^ 1) - 1) for i in range(space_count)],
            )
        ]
        even = space_rank % 2 == 0
        send = jnp.where(even, jnp.roll(send_list, half, axis=1), send_list)
        swapped = neighbours + jnp.where(neighbours < node_count + half, half, -half)
        near = jnp.where(even & (neighbours >= node_count), swapped, neighbours)
        low, high = space_rank > 0, space_rank < ends
        edges = jnp.stack([jnp.where(even, high, low), jnp.where(even, low, high)])
        edges = edges.astype(jnp.float32)

        thick = jnp.broadcast_to(thickness[:, None], (held, LANES))
        own = jnp.concatenate([velocity[0], velocity[1], density, thick], axis=1)
        parts = lax.all_gather(own, "level")
        thick = parts[:, :, 3 * node_count :].reshape(level_count, LANES)
        pad = -near_count % SUBS
        near = jnp.pad(near, ((0, pad), (0, 0)))
        weights = jnp.concatenate([grad_weights, lap_weights[None]], axis=0)
        weights = jnp.pad(weights, ((0, 0), (0, pad), (0, 0)))
        eta = elevation[None]
        depth = bottom[None]
        area = node_area[None]
        out_shape = shape(2, rows + SUBS, half)

        state, outgoing, volume = pl.pallas_call(
            begin_kernel,
            out_shape=(shape(rows, node_count), out_shape, shape(SUBS, LANES)),
            in_specs=vmem(5),
            out_specs=tuple(vmem(3)),
            name="begin",
        )(parts, eta, depth, area, send)

        for step in range(STEPS):
            halos = [lax.ppermute(outgoing[i], "space", rounds[i]) for i in range(2)]

            def body(*refs, step=step):
                step_kernel(*refs, near_count=near_count, step=step)

            state, eta, outgoing, volume = pl.pallas_call(
                body,
                out_shape=(
                    shape(rows, node_count),
                    shape(1, node_count),
                    out_shape,
                    shape(SUBS, LANES),
                ),
                in_specs=[pl.BlockSpec(memory_space=pltpu.SMEM)] + vmem(12),
                out_specs=tuple(vmem(4)),
                name="step",
            )(
                edges, volume, state, eta, *halos, near, weights,
                coriolis[None], area, depth, thick, send,
            )

        shared = jnp.broadcast_to(volume, (space_count,) + volume.shape)
        shared = lax.all_to_all(shared, "space", 0, 0)
        summed = jnp.sum(shared, axis=(0, 2))
        drifts = summed[:STEPS] / summed[STEPS]
        eta = eta[0] + time_step * jnp.sum(drifts)
        fields = state.reshape(3, level_count, node_count)
        mine = lax.dynamic_slice_in_dim(fields, level_rank * held, held, axis=1)
        return mine[:2], mine[2], eta, drifts

    return local


def solution(mesh):
    return jax.shard_map(
        make_local(mesh),
        mesh=mesh,
        in_specs=(
            P(None, "level", "space"),
            P("level", "space"),
            P("space"),
            P(None, None, "space"),
            P(None, "space"),
            P("space"),
            P("space"),
            P("level"),
            P("space", None),
            P(None, "space"),
            P("space"),
        ),
        out_specs=(P(None, "level", "space"), P("level", "space"), P("space"), P()),
        check_vma=False,
    )
```

```python
import jax
import jax.numpy as jnp
from jax import lax
from jax.experimental import pallas as pl
from jax.experimental.pallas import tpu as pltpu
from jax.sharding import PartitionSpec as P

STEPS = 4

time_step = 0.1
buoyancy = 0.5
drag_rate = 0.5

LANES = 128
SUBS = 8


def lane_gather(source, lane):
    return lax.gather(
        source,
        lane[..., None],
        lax.GatherDimensionNumbers(
            offset_dims=(),
            collapsed_slice_dims=(1,),
            start_index_map=(1,),
            operand_batching_dims=(0,),
            start_indices_batching_dims=(0,),
        ),
        slice_sizes=(1, 1),
        mode=lax.GatherScatterMode.PROMISE_IN_BOUNDS,
    )


def spread(row, rows=SUBS):
    return jnp.broadcast_to(row, (rows, row.shape[1]))


def level_prefix(value):
    sub = lax.broadcasted_iota(jnp.int32, (SUBS, LANES), 0)
    out, carry = [], None
    for block in value:
        shift = 1
        while shift < SUBS:
            block = block + jnp.where(sub >= shift, pltpu.roll(block, shift, 0), 0.0)
            shift *= 2
        if carry is not None:
            block = block + carry
        carry = spread(block[SUBS - 1 :])
        out.append(block)
    return out


def pick(sources, lane, block):
    out = None
    for number, rows in enumerate(sources):
        here = [lane_gather(row(), lane) for row in rows]
        if out is None:
            out = here
        else:
            match = block == number
            out = [jnp.where(match, new, old) for new, old in zip(here, out)]
    return out


def send_out(even, state, eta, send, outgoing):
    rows, node_count = state.shape
    half = send.shape[1] // 2
    for side in range(2):
        for chunk in range(half // LANES):
            low = chunk * LANES
            lower, upper = (send[0:1, i : i + LANES] for i in (low, half + low))
            if side:
                lower, upper = upper, lower
            ids = spread(jnp.where(even, upper, lower))
            sources = []
            for number in range(node_count // LANES):
                cols = slice(number * LANES, (number + 1) * LANES)
                own = [
                    lambda g=g, cols=cols: state[g : g + SUBS, cols]
                    for g in range(0, rows, SUBS)
                ]
                own.append(lambda cols=cols: spread(eta[0:1, cols]))
                sources.append(own)
            found = pick(sources, ids & (LANES - 1), ids >> 7)
            for g, block in enumerate(found):
                outgoing[side][g * SUBS : (g + 1) * SUBS, low : low + LANES] = block


def prepare_kernel(flags, neighbours, grad_weights, lap_weights, near, weights):
    near_count, node_count = neighbours.shape
    half = (flags[3] - node_count) // 2
    ids = neighbours[...]
    first_ok, second_ok = (jnp.where(flags[i] > 0, 1.0, 0.0) for i in (1, 2))
    own, low = ids < node_count, ids < node_count + half
    swapped = jnp.where(own, ids, jnp.where(low, ids + half, ids - half))
    ids = jnp.where(flags[0] > 0, swapped, ids)
    valid = jnp.where(own, 1.0, jnp.where(ids < node_count + half, first_ok, second_ok))
    near[...] = jnp.zeros(near.shape, jnp.int32)
    weights[...] = jnp.zeros(weights.shape, jnp.float32)
    near[:near_count, :] = ids
    weights[0, :near_count, :] = grad_weights[0] * valid
    weights[1, :near_count, :] = grad_weights[1] * valid
    weights[2, :near_count, :] = lap_weights[...] * valid


def begin_kernel(
    flags, parts, eta, bottom, node_area, send, state, first_out, second_out, volume
):
    shards, held, width = parts.shape
    fields, node_count = 3, eta.shape[1]
    level_count = shards * held
    area = jnp.where(bottom[0:1, :] > 0, node_area[0:1, :], 0.0)
    area = sum(area[:, i : i + LANES] for i in range(0, node_count, LANES))
    sub = lax.broadcasted_iota(jnp.int32, (SUBS, LANES), 0)
    volume[...] = jnp.where(sub == STEPS, spread(area), 0.0)
    for shard in range(shards):
        ids = lax.broadcasted_iota(jnp.int32, (held, node_count), 0) + shard * held
        wet = ids < jnp.broadcast_to(bottom[0:1, :], (held, node_count))
        for field in range(fields):
            value = parts[shard, :, field * node_count : (field + 1) * node_count]
            if field < 2:
                value = jnp.where(wet, value, 0.0)
            first = field * level_count + shard * held
            state[first : first + held, :] = value
    send_out(flags[0] > 0, state, eta, send, (first_out, second_out))


def step_kernel(
    flags,
    volume_in,
    state,
    eta,
    first_halo,
    second_halo,
    neighbours,
    weights,
    coriolis,
    node_area,
    bottom,
    thickness,
    send,
    *outputs,
    near_count,
    step,
):
    last = step == STEPS - 1
    if last:
        velocity_out, density_out, new_eta, volume, new_state = outputs
    else:
        new_state, new_eta, first_out, second_out, volume = outputs
    rows, node_count = state.shape
    half = first_halo.shape[1]
    level_count = rows // 3
    groups = level_count // SUBS

    def source_blocks():
        for ref, width in ((state, node_count), (first_halo, half), (second_halo, half)):
            for number in range(width // LANES):
                cols = slice(number * LANES, (number + 1) * LANES)
                yield ref, cols

    eta_sources, state_sources = [], []
    for ref, cols in source_blocks():
        eta_ref, eta_row = (eta, 0) if ref is state else (ref, rows)
        eta_sources.append(
            [lambda r=eta_ref, i=eta_row, c=cols: spread(r[i : i + 1, c])]
        )
        state_sources.append(
            [lambda r=ref, g=g, c=cols: r[g : g + SUBS, c] for g in range(0, rows, SUBS)]
        )

    sub = lax.broadcasted_iota(jnp.int32, (SUBS, LANES), 0)

    def tile(number, total):
        cols = pl.ds(pl.multiple_of(number * LANES, LANES), LANES)
        ids = neighbours[:, cols]
        lanes, blocks = ids & (LANES - 1), ids >> 7
        east, north, smooth = (weights[i, :, cols] for i in range(3))
        eta_here = eta[0:1, cols]
        (eta_near,) = pick(eta_sources, lanes, blocks)
        eta_differ = eta_near - spread(eta_here)
        slope_east = spread(jnp.sum(east * eta_differ, axis=0, keepdims=True))
        slope_north = spread(jnp.sum(north * eta_differ, axis=0, keepdims=True))

        own = [state[g : g + SUBS, cols] for g in range(0, rows, SUBS)]
        zero = jnp.zeros((SUBS, LANES), jnp.float32)
        lap = [zero] * (3 * groups)
        flow = [zero] * groups
        dense_east = [zero] * groups
        dense_north = [zero] * groups
        for k in range(near_count):
            found = pick(state_sources, spread(lanes[k : k + 1]), spread(blocks[k : k + 1]))
            e, n, w = (spread(x[k : k + 1]) for x in (east, north, smooth))
            differ = [near - here for near, here in zip(found, own)]
            for i, value in enumerate(differ):
                lap[i] = lap[i] + w * value
            for g in range(groups):
                flow[g] = flow[g] + (e * differ[g] + n * differ[groups + g])
                dense_east[g] = dense_east[g] + e * differ[2 * groups + g]
                dense_north[g] = dense_north[g] + n * differ[2 * groups + g]

        thick = [thickness[g * SUBS : (g + 1) * SUBS, :] for g in range(groups)]
        diverge = sum(thick[g] * flow[g] for g in range(groups))
        diverge = jnp.sum(diverge, axis=0, keepdims=True)
        depth = bottom[0:1, cols]
        wet_nodes = jnp.where(depth > 0, 1.0, 0.0)
        total = total + node_area[0:1, cols] * wet_nodes * diverge
        new_eta[0:1, cols] = eta_here - time_step * wet_nodes * diverge

        weighted_east = [t * x for t, x in zip(thick, dense_east)]
        weighted_north = [t * x for t, x in zip(thick, dense_north)]
        press_east = level_prefix(weighted_east)
        press_north = level_prefix(weighted_north)
        turn = spread(coriolis[0:1, cols])
        depth = spread(depth)
        for g in range(groups):
            u, v, rho = (own[f * groups + g] for f in range(3))
            level = sub + g * SUBS
            wet = level < depth
            drag = jnp.where(level == depth - 1, drag_rate, 0.0)
            push_east = (
                lap[g]
                - slope_east
                - buoyancy * (press_east[g] - 0.5 * weighted_east[g])
                + turn * v
                - drag * u
            )
            push_north = (
                lap[groups + g]
                - slope_north
                - buoyancy * (press_north[g] - 0.5 * weighted_north[g])
                - turn * u
                - drag * v
            )
            rho_new = rho + time_step * (
                lap[2 * groups + g] - u * dense_east[g] - v * dense_north[g]
            )
            u_new = jnp.where(wet, u + time_step * push_east, 0.0)
            v_new = jnp.where(wet, v + time_step * push_north, 0.0)
            for f, value in enumerate((u_new, v_new, rho_new)):
                first = (f * groups + g) * SUBS
                new_state[first : first + SUBS, cols] = value
        return total

    total = lax.fori_loop(
        0, node_count // LANES, tile, jnp.zeros((1, LANES), jnp.float32)
    )
    volume[...] = jnp.where(sub == step, spread(total), volume_in[...])
    if last:
        held = density_out.shape[0]
        for field in range(3):
            first = pl.multiple_of(field * level_count + flags[4] * held, SUBS)
            value = new_state[pl.ds(first, held), :]
            if field < 2:
                velocity_out[field] = value
            else:
                density_out[...] = value
    else:
        send_out(flags[0] > 0, new_state, new_eta, send, (first_out, second_out))


def vmem(count):
    return [pl.BlockSpec(memory_space=pltpu.VMEM)] * count


def kept(*dims, dtype=jnp.float32):
    return pltpu.VMEM(dims, dtype)


def keep(array):
    return pltpu.with_memory_space_constraint(array, pltpu.VMEM)


def shape(*dims):
    return jax.ShapeDtypeStruct(dims, jnp.float32)


def make_local(mesh):
    def local(
        velocity,
        density,
        elevation,
        grad_weights,
        lap_weights,
        coriolis,
        node_area,
        thickness,
        send_list,
        neighbours,
        bottom,
    ):
        held, node_count = density.shape
        near_count = neighbours.shape[0]
        half = send_list.shape[1] // 2
        shards = mesh.shape["level"]
        space_count = mesh.shape["space"]
        level_count = shards * held
        rows = 3 * level_count
        space_rank = lax.axis_index("space")
        level_rank = lax.axis_index("level")
        ends = space_count - 1
        rounds = [
            [(i, j if 0 <= j <= ends else i) for i, j in pairs]
            for pairs in (
                [(i, i ^ 1) for i in range(space_count)],
                [(i, ((i + 1) ^ 1) - 1) for i in range(space_count)],
            )
        ]
        even = space_rank % 2 == 0
        low, high = space_rank > 0, space_rank < ends
        flags = jnp.stack(
            [
                even.astype(jnp.int32),
                jnp.where(even, high, low).astype(jnp.int32),
                jnp.where(even, low, high).astype(jnp.int32),
                jnp.int32(node_count + 2 * half),
                level_rank.astype(jnp.int32),
            ]
        )

        thick = jnp.broadcast_to(thickness[:, None], (held, LANES))
        own = jnp.concatenate([velocity[0], velocity[1], density, thick], axis=1)
        parts = lax.all_gather(own, "level")
        thick = parts[:, :, 3 * node_count :].reshape(level_count, LANES)
        pad = -near_count % SUBS
        near_rows = near_count + pad
        eta = elevation[None]
        depth = bottom[None]
        area = node_area[None]
        scalars = [pl.BlockSpec(memory_space=pltpu.SMEM)]
        halo = (rows + SUBS, half)

        state, *outgoing, volume = pl.pallas_call(
            begin_kernel,
            out_shape=(kept(rows, node_count), kept(*halo), kept(*halo), kept(SUBS, LANES)),
            in_specs=scalars + vmem(5),
            out_specs=tuple(vmem(4)),
            name="begin",
        )(flags, parts, eta, depth, area, send_list)
        near, weights = pl.pallas_call(
            prepare_kernel,
            out_shape=(
                kept(near_rows, node_count, dtype=jnp.int32),
                kept(3, near_rows, node_count),
            ),
            in_specs=scalars + vmem(3),
            out_specs=tuple(vmem(2)),
            name="prepare",
        )(flags, neighbours, grad_weights, lap_weights)
        fixed = (near, weights, coriolis[None], area, depth, thick, send_list)
        fixed = tuple(map(keep, fixed))

        for step in range(STEPS):
            halos = [
                keep(lax.ppermute(value, "space", pairs))
                for value, pairs in zip(outgoing, rounds)
            ]

            def body(*refs, step=step):
                step_kernel(*refs, near_count=near_count, step=step)

            last = step == STEPS - 1
            if last:
                outs = (
                    shape(2, held, node_count),
                    shape(held, node_count),
                    kept(1, node_count),
                    kept(SUBS, LANES),
                )
                scratch = [pltpu.VMEM((rows, node_count), jnp.float32)]
            else:
                outs = (
                    kept(rows, node_count),
                    kept(1, node_count),
                    kept(*halo),
                    kept(*halo),
                    kept(SUBS, LANES),
                )
                scratch = []
            results = pl.pallas_call(
                body,
                out_shape=outs,
                in_specs=scalars + vmem(12),
                out_specs=tuple(vmem(len(outs))),
                scratch_shapes=scratch,
                name="step",
            )(flags, *map(keep, (volume, state, eta)), *halos, *fixed)
            if last:
                velocity_out, density_out, eta, volume = results
            else:
                state, eta, *outgoing, volume = results

        if space_count & (space_count - 1):
            volume = lax.psum(volume, "space")
        else:
            distance = 1
            while distance < space_count:
                pairs = [(i, i ^ distance) for i in range(space_count)]
                volume = volume + lax.ppermute(volume, "space", pairs)
                distance *= 2
        summed = jnp.sum(volume, axis=1)
        drifts = summed[:STEPS] / summed[STEPS]
        eta = eta[0] + time_step * jnp.sum(drifts)
        return velocity_out, density_out, eta, drifts

    return local


def solution(mesh):
    return jax.shard_map(
        make_local(mesh),
        mesh=mesh,
        in_specs=(
            P(None, "level", "space"),
            P("level", "space"),
            P("space"),
            P(None, None, "space"),
            P(None, "space"),
            P("space"),
            P("space"),
            P("level"),
            P("space", None),
            P(None, "space"),
            P("space"),
        ),
        out_specs=(P(None, "level", "space"), P("level", "space"), P("space"), P()),
        check_vma=False,
    )
```

```python
import jax
import jax.numpy as jnp
from jax import lax
from jax.experimental import pallas as pl
from jax.experimental.pallas import tpu as pltpu
from jax.sharding import PartitionSpec as P

STEPS = 4

time_step = 0.1
buoyancy = 0.5
drag_rate = 0.5

LANES = 128
SUBS = 8


def lane_gather(source, lane):
    return lax.gather(
        source,
        lane[..., None],
        lax.GatherDimensionNumbers(
            offset_dims=(),
            collapsed_slice_dims=(1,),
            start_index_map=(1,),
            operand_batching_dims=(0,),
            start_indices_batching_dims=(0,),
        ),
        slice_sizes=(1, 1),
        mode=lax.GatherScatterMode.PROMISE_IN_BOUNDS,
    )


def spread(row, rows=SUBS):
    return jnp.broadcast_to(row, (rows, row.shape[1]))


def level_prefix(value):
    sub = lax.broadcasted_iota(jnp.int32, (SUBS, LANES), 0)
    out, carry = [], None
    for block in value:
        shift = 1
        while shift < SUBS:
            block = block + jnp.where(sub >= shift, pltpu.roll(block, shift, 0), 0.0)
            shift *= 2
        if carry is not None:
            block = block + carry
        carry = spread(block[SUBS - 1 :])
        out.append(block)
    return out


def pick(sources, lane, block):
    out = None
    for number, rows in enumerate(sources):
        here = [lane_gather(row(), lane) for row in rows]
        if out is None:
            out = here
        else:
            match = block == number
            out = [jnp.where(match, new, old) for new, old in zip(here, out)]
    return out


def send_out(even, state, eta, send, outgoing):
    rows, node_count = state.shape
    half = send.shape[1] // 2
    for side in range(2):
        for chunk in range(half // LANES):
            low = chunk * LANES
            lower, upper = (send[0:1, i : i + LANES] for i in (low, half + low))
            if side:
                lower, upper = upper, lower
            ids = spread(jnp.where(even, upper, lower))
            sources = []
            for number in range(node_count // LANES):
                cols = slice(number * LANES, (number + 1) * LANES)
                own = [
                    lambda g=g, cols=cols: state[g : g + SUBS, cols]
                    for g in range(0, rows, SUBS)
                ]
                own.append(lambda cols=cols: spread(eta[0:1, cols]))
                sources.append(own)
            found = pick(sources, ids & (LANES - 1), ids >> 7)
            for g, block in enumerate(found):
                outgoing[side][g * SUBS : (g + 1) * SUBS, low : low + LANES] = block


def prepare_kernel(flags, neighbours, grad_weights, lap_weights, near, weights):
    near_count, node_count = neighbours.shape
    half = (flags[3] - node_count) // 2
    ids = neighbours[...]
    first_ok, second_ok = (jnp.where(flags[i] > 0, 1.0, 0.0) for i in (1, 2))
    own, low = ids < node_count, ids < node_count + half
    swapped = jnp.where(own, ids, jnp.where(low, ids + half, ids - half))
    ids = jnp.where(flags[0] > 0, swapped, ids)
    valid = jnp.where(own, 1.0, jnp.where(ids < node_count + half, first_ok, second_ok))
    near[...] = jnp.zeros(near.shape, jnp.int32)
    weights[...] = jnp.zeros(weights.shape, jnp.float32)
    near[:near_count, :] = ids
    weights[0, :near_count, :] = grad_weights[0] * valid
    weights[1, :near_count, :] = grad_weights[1] * valid
    weights[2, :near_count, :] = lap_weights[...] * valid


def begin_kernel(
    flags, parts, eta, bottom, node_area, send, state, first_out, second_out, volume
):
    shards, held, width = parts.shape
    fields, node_count = 3, eta.shape[1]
    level_count = shards * held
    area = jnp.where(bottom[0:1, :] > 0, node_area[0:1, :], 0.0)
    area = sum(area[:, i : i + LANES] for i in range(0, node_count, LANES))
    sub = lax.broadcasted_iota(jnp.int32, (SUBS, LANES), 0)
    volume[...] = jnp.where(sub == STEPS, spread(area), 0.0)
    for shard in range(shards):
        ids = lax.broadcasted_iota(jnp.int32, (held, node_count), 0) + shard * held
        wet = ids < jnp.broadcast_to(bottom[0:1, :], (held, node_count))
        for field in range(fields):
            value = parts[shard, :, field * node_count : (field + 1) * node_count]
            if field < 2:
                value = jnp.where(wet, value, 0.0)
            first = field * level_count + shard * held
            state[first : first + held, :] = value
    send_out(flags[0] > 0, state, eta, send, (first_out, second_out))


def step_kernel(
    flags,
    volume_in,
    state,
    eta,
    first_halo,
    second_halo,
    neighbours,
    weights,
    coriolis,
    node_area,
    bottom,
    thickness,
    send,
    *outputs,
    near_count,
    step,
):
    last = step == STEPS - 1
    if last:
        velocity_out, density_out, new_eta, volume, new_state = outputs
    else:
        new_state, new_eta, first_out, second_out, volume = outputs
    rows, node_count = state.shape
    half = first_halo.shape[1]
    level_count = rows // 3
    groups = level_count // SUBS

    def source_blocks():
        for ref, width in ((state, node_count), (first_halo, half), (second_halo, half)):
            for number in range(width // LANES):
                cols = slice(number * LANES, (number + 1) * LANES)
                yield ref, cols

    eta_sources, state_sources = [], []
    for ref, cols in source_blocks():
        eta_ref, eta_row = (eta, 0) if ref is state else (ref, rows)
        eta_sources.append(
            [lambda r=eta_ref, i=eta_row, c=cols: spread(r[i : i + 1, c])]
        )
        state_sources.append(
            [lambda r=ref, g=g, c=cols: r[g : g + SUBS, c] for g in range(0, rows, SUBS)]
        )

    sub = lax.broadcasted_iota(jnp.int32, (SUBS, LANES), 0)

    def tile(number, total):
        cols = pl.ds(pl.multiple_of(number * LANES, LANES), LANES)
        ids = neighbours[:, cols]
        lanes, blocks = ids & (LANES - 1), ids >> 7
        east, north, smooth = (weights[i, :, cols] for i in range(3))
        eta_here = eta[0:1, cols]
        (eta_near,) = pick(eta_sources, lanes, blocks)
        eta_differ = eta_near - spread(eta_here)
        slope_east = spread(jnp.sum(east * eta_differ, axis=0, keepdims=True))
        slope_north = spread(jnp.sum(north * eta_differ, axis=0, keepdims=True))

        own = [state[g : g + SUBS, cols] for g in range(0, rows, SUBS)]
        zero = jnp.zeros((SUBS, LANES), jnp.float32)
        lap = [zero] * (3 * groups)
        flow = [zero] * groups
        dense_east = [zero] * groups
        dense_north = [zero] * groups
        for k in range(near_count):
            found = pick(state_sources, spread(lanes[k : k + 1]), spread(blocks[k : k + 1]))
            e, n, w = (spread(x[k : k + 1]) for x in (east, north, smooth))
            differ = [near - here for near, here in zip(found, own)]
            for i, value in enumerate(differ):
                lap[i] = lap[i] + w * value
            for g in range(groups):
                flow[g] = flow[g] + (e * differ[g] + n * differ[groups + g])
                dense_east[g] = dense_east[g] + e * differ[2 * groups + g]
                dense_north[g] = dense_north[g] + n * differ[2 * groups + g]

        thick = [thickness[g * SUBS : (g + 1) * SUBS, :] for g in range(groups)]
        diverge = sum(thick[g] * flow[g] for g in range(groups))
        diverge = jnp.sum(diverge, axis=0, keepdims=True)
        depth = bottom[0:1, cols]
        wet_nodes = jnp.where(depth > 0, 1.0, 0.0)
        total = total + node_area[0:1, cols] * wet_nodes * diverge
        new_eta[0:1, cols] = eta_here - time_step * wet_nodes * diverge

        weighted_east = [t * x for t, x in zip(thick, dense_east)]
        weighted_north = [t * x for t, x in zip(thick, dense_north)]
        press_east = level_prefix(weighted_east)
        press_north = level_prefix(weighted_north)
        turn = spread(coriolis[0:1, cols])
        depth = spread(depth)
        for g in range(groups):
            u, v, rho = (own[f * groups + g] for f in range(3))
            level = sub + g * SUBS
            wet = level < depth
            drag = jnp.where(level == depth - 1, drag_rate, 0.0)
            push_east = (
                lap[g]
                - slope_east
                - buoyancy * (press_east[g] - 0.5 * weighted_east[g])
                + turn * v
                - drag * u
            )
            push_north = (
                lap[groups + g]
                - slope_north
                - buoyancy * (press_north[g] - 0.5 * weighted_north[g])
                - turn * u
                - drag * v
            )
            rho_new = rho + time_step * (
                lap[2 * groups + g] - u * dense_east[g] - v * dense_north[g]
            )
            u_new = jnp.where(wet, u + time_step * push_east, 0.0)
            v_new = jnp.where(wet, v + time_step * push_north, 0.0)
            for f, value in enumerate((u_new, v_new, rho_new)):
                first = (f * groups + g) * SUBS
                new_state[first : first + SUBS, cols] = value
        return total

    total = lax.fori_loop(
        0, node_count // LANES, tile, jnp.zeros((1, LANES), jnp.float32)
    )
    volume[...] = jnp.where(sub == step, spread(total), volume_in[...])
    if last:
        held = density_out.shape[0]
        for field in range(3):
            first = pl.multiple_of(field * level_count + flags[4] * held, SUBS)
            value = new_state[pl.ds(first, held), :]
            if field < 2:
                velocity_out[field] = value
            else:
                density_out[...] = value
    else:
        send_out(flags[0] > 0, new_state, new_eta, send, (first_out, second_out))


def finish_kernel(volume, eta, eta_out, drifts):
    summed = jnp.sum(volume[...], axis=1, keepdims=True)
    ratio = summed / summed[STEPS : STEPS + 1, :]
    eta_out[...] = eta[...] + time_step * jnp.sum(ratio[:STEPS], axis=0, keepdims=True)
    drifts[...] = jnp.broadcast_to(ratio, drifts.shape)


def vmem(count):
    return [pl.BlockSpec(memory_space=pltpu.VMEM)] * count


def kept(*dims, dtype=jnp.float32):
    return pltpu.VMEM(dims, dtype)


def keep(array):
    return pltpu.with_memory_space_constraint(array, pltpu.VMEM)


def shape(*dims):
    return jax.ShapeDtypeStruct(dims, jnp.float32)


def make_local(mesh):
    def local(
        velocity,
        density,
        elevation,
        grad_weights,
        lap_weights,
        coriolis,
        node_area,
        thickness,
        send_list,
        neighbours,
        bottom,
    ):
        held, node_count = density.shape
        near_count = neighbours.shape[0]
        half = send_list.shape[1] // 2
        shards = mesh.shape["level"]
        space_count = mesh.shape["space"]
        level_count = shards * held
        rows = 3 * level_count
        space_rank = lax.axis_index("space")
        level_rank = lax.axis_index("level")
        ends = space_count - 1
        rounds = [
            [(i, j if 0 <= j <= ends else i) for i, j in pairs]
            for pairs in (
                [(i, i ^ 1) for i in range(space_count)],
                [(i, ((i + 1) ^ 1) - 1) for i in range(space_count)],
            )
        ]
        even = space_rank % 2 == 0
        low, high = space_rank > 0, space_rank < ends
        flags = jnp.stack(
            [
                even.astype(jnp.int32),
                jnp.where(even, high, low).astype(jnp.int32),
                jnp.where(even, low, high).astype(jnp.int32),
                jnp.int32(node_count + 2 * half),
                level_rank.astype(jnp.int32),
            ]
        )

        thick = jnp.broadcast_to(thickness[:, None], (held, LANES))
        own = jnp.concatenate([velocity[0], velocity[1], density, thick], axis=1)
        parts = lax.all_gather(own, "level")
        thick = parts[:, :, 3 * node_count :].reshape(level_count, LANES)
        pad = -near_count % SUBS
        near_rows = near_count + pad
        eta = elevation[None]
        depth = bottom[None]
        area = node_area[None]
        scalars = [pl.BlockSpec(memory_space=pltpu.SMEM)]
        halo = (rows + SUBS, half)

        state, *outgoing, volume = pl.pallas_call(
            begin_kernel,
            out_shape=(kept(rows, node_count), kept(*halo), kept(*halo), kept(SUBS, LANES)),
            in_specs=scalars + vmem(5),
            out_specs=tuple(vmem(4)),
            name="begin",
        )(flags, parts, eta, depth, area, send_list)
        near, weights = pl.pallas_call(
            prepare_kernel,
            out_shape=(
                kept(near_rows, node_count, dtype=jnp.int32),
                kept(3, near_rows, node_count),
            ),
            in_specs=scalars + vmem(3),
            out_specs=tuple(vmem(2)),
            name="prepare",
        )(flags, neighbours, grad_weights, lap_weights)
        fixed = (near, weights, coriolis[None], area, depth, thick, send_list)
        fixed = tuple(map(keep, fixed))

        for step in range(STEPS):
            halos = [
                keep(lax.ppermute(value, "space", pairs))
                for value, pairs in zip(outgoing, rounds)
            ]

            def body(*refs, step=step):
                step_kernel(*refs, near_count=near_count, step=step)

            last = step == STEPS - 1
            if last:
                outs = (
                    shape(2, held, node_count),
                    shape(held, node_count),
                    kept(1, node_count),
                    kept(SUBS, LANES),
                )
                scratch = [pltpu.VMEM((rows, node_count), jnp.float32)]
            else:
                outs = (
                    kept(rows, node_count),
                    kept(1, node_count),
                    kept(*halo),
                    kept(*halo),
                    kept(SUBS, LANES),
                )
                scratch = []
            results = pl.pallas_call(
                body,
                out_shape=outs,
                in_specs=scalars + vmem(12),
                out_specs=tuple(vmem(len(outs))),
                scratch_shapes=scratch,
                name="step",
            )(flags, *map(keep, (volume, state, eta)), *halos, *fixed)
            if last:
                velocity_out, density_out, eta, volume = results
            else:
                state, eta, *outgoing, volume = results

        if space_count & (space_count - 1):
            volume = lax.psum(volume, "space")
        else:
            distance = 1
            while distance < space_count:
                pairs = [(i, i ^ distance) for i in range(space_count)]
                volume = volume + lax.ppermute(volume, "space", pairs)
                distance *= 2
        eta, drifts = pl.pallas_call(
            finish_kernel,
            out_shape=(shape(1, node_count), shape(SUBS, LANES)),
            in_specs=vmem(2),
            out_specs=tuple(vmem(2)),
            name="finish",
        )(keep(volume), keep(eta))
        return velocity_out, density_out, eta[0], drifts[:STEPS, 0]

    return local


def solution(mesh):
    return jax.shard_map(
        make_local(mesh),
        mesh=mesh,
        in_specs=(
            P(None, "level", "space"),
            P("level", "space"),
            P("space"),
            P(None, None, "space"),
            P(None, "space"),
            P("space"),
            P("space"),
            P("level"),
            P("space", None),
            P(None, "space"),
            P("space"),
        ),
        out_specs=(P(None, "level", "space"), P("level", "space"), P("space"), P()),
        check_vma=False,
    )
```
